32 devices in a mesh: dp: 1 (over z), tp: 32 (over y, x, core).
Axes of the slice: x: 4, y: 4, z: 1, core: 2. Of those that a mesh axis runs over, the one named last changes fastest.
The devices are a block of a 4x4x8 slice.
Arguments:
- hidden: bfloat16 [16384, 1536], P(('dp', 'tp'))
- ln_gain: float32 [1536], replicated
- ln_bias: float32 [1536], replicated
- embed: bfloat16 [16384, 1536], P('tp')
- targets: int32 [16384], P(('dp', 'tp'))
- loss_mask: int32 [16384], P(('dp', 'tp'))
Outputs:
- output 1: float32 [16384], P(('dp', 'tp'))
- output 2: float32 [1], P('dp')
- output 3: bfloat16 [16384, 1536], P(('dp', 'tp'))
- output 4: float32 [16384, 1536], P(('dp', 'tp'))
- output 5: float32 [1536], P('dp')
- output 6: float32 [1536], P('dp')
All inputs are finite; a program needn't handle non-finite values.
Results may differ from the reference program's by a relative error of at most 0.001.
Values are sent between devices in bfloat16 or wider.
A program may use at most 768 MiB of HBM per device.

```python
import jax
import jax.numpy as jnp
from jax import lax

TOKENS_DEV = 512
GROUP_SIZE = 32
MODEL_DIM = 1536
VOCAB_SIZE = 16384
LN_EPS = 1e-5


def setup_inputs(seed: int = 0, part: int = 0) -> dict:
    seq_len = GROUP_SIZE * TOKENS_DEV
    part_keys = jax.random.split(jax.random.fold_in(jax.random.key(seed), part), 4)
    shared_keys = jax.random.split(jax.random.key(seed + 1), 3)
    embed_scale = 2.5 * MODEL_DIM ** -0.5
    hidden = jax.random.normal(part_keys[0], (seq_len, MODEL_DIM), jnp.float32).astype(jnp.bfloat16)
    ln_gain = 1.0 + 0.3 * jax.random.normal(shared_keys[0], (MODEL_DIM,), jnp.float32)
    ln_bias = 0.3 * jax.random.normal(shared_keys[1], (MODEL_DIM,), jnp.float32)
    embed = (embed_scale * jax.random.normal(shared_keys[2], (VOCAB_SIZE, MODEL_DIM), jnp.float32)).astype(jnp.bfloat16)
    targets = jax.random.randint(part_keys[1], (seq_len,), 0, VOCAB_SIZE, dtype=jnp.int32)
    shard_rate = jax.random.randint(part_keys[2], (GROUP_SIZE, 1), 40, 96, dtype=jnp.int32)
    draws = jax.random.randint(part_keys[3], (GROUP_SIZE, TOKENS_DEV), 0, 100, dtype=jnp.int32)
    loss_mask = (draws < shard_rate).astype(jnp.int32).reshape(seq_len)
    return {'hidden': hidden, 'ln_gain': ln_gain, 'ln_bias': ln_bias, 'embed': embed, 'targets': targets, 'loss_mask': loss_mask}


def normalize(hidden):
    h_f32 = hidden.astype(jnp.float32)
    centred = h_f32 - jnp.mean(h_f32, axis=-1, keepdims=True)
    inv_std = lax.rsqrt(jnp.mean(centred * centred, axis=-1, keepdims=True) + LN_EPS)
    return centred * inv_std, inv_std


def reference(hidden, ln_gain, ln_bias, embed, targets, loss_mask):
    seq_len = GROUP_SIZE * TOKENS_DEV
    x_hat, inv_std = normalize(hidden)
    normed = (x_hat * ln_gain + ln_bias).astype(jnp.bfloat16)
    weights = loss_mask.astype(jnp.float32)
    count = jnp.sum(weights)
    vocab_ids = jnp.arange(VOCAB_SIZE, dtype=jnp.int32)

    def block_step(embed_acc, block):
        x_blk, t_blk, w_blk = block
        logits = jnp.dot(x_blk, embed.T, preferred_element_type=jnp.float32)
        row_max = jnp.max(logits, axis=-1, keepdims=True)
        log_norm = row_max[:, 0] + jnp.log(jnp.sum(jnp.exp(logits - row_max), axis=-1))
        onehot = (vocab_ids[None, :] == t_blk[:, None]).astype(jnp.float32)
        t_logit = jnp.sum(logits * onehot, axis=-1)
        loss_blk = (log_norm - t_logit) * w_blk
        d_logits = ((jnp.exp(logits - log_norm[:, None]) - onehot) * (w_blk / count)[:, None]).astype(jnp.bfloat16)
        embed_acc = embed_acc + jnp.dot(d_logits.T, x_blk, preferred_element_type=jnp.float32)
        d_x = jnp.dot(d_logits, embed, preferred_element_type=jnp.float32)
        return embed_acc, (loss_blk, d_x)

    blocks = (normed.reshape(GROUP_SIZE, TOKENS_DEV, MODEL_DIM), targets.reshape(GROUP_SIZE, TOKENS_DEV), weights.reshape(GROUP_SIZE, TOKENS_DEV))
    d_embed, outs = lax.scan(block_step, jnp.zeros((VOCAB_SIZE, MODEL_DIM), jnp.float32), blocks)
    loss = outs[0].reshape(seq_len)
    d_normed = outs[1].reshape(seq_len, MODEL_DIM)
    mean_loss = jnp.sum(loss) / count
    d_gain = jnp.sum(d_normed * x_hat, axis=0)
    d_bias = jnp.sum(d_normed, axis=0)
    d_xhat = d_normed * ln_gain
    centre_term = jnp.mean(d_xhat, axis=-1, keepdims=True)
    proj_term = jnp.mean(d_xhat * x_hat, axis=-1, keepdims=True)
    d_hidden = (inv_std * (d_xhat - centre_term - x_hat * proj_term)).astype(jnp.bfloat16)
    return loss, mean_loss.reshape(1), d_hidden, d_embed, d_gain, d_bias
```

```python
import functools

import jax
import jax.numpy as jnp
from jax import lax
from jax.experimental import pallas as pl
from jax.experimental.pallas import tpu as pltpu
from jax.sharding import PartitionSpec as P

LN_EPS = 1e-5
CORES = 2
SIDE = 4
OFFSETS = (0, -1, 1, 2)
VMEM_LIMIT = 60 * 1024 * 1024
MESH = pl.DeviceIdType.MESH


def normalize(hidden):
    h_f32 = hidden.astype(jnp.float32)
    centred = h_f32 - jnp.mean(h_f32, axis=-1, keepdims=True)
    inv_std = lax.rsqrt(jnp.mean(centred * centred, axis=-1, keepdims=True) + LN_EPS)
    return centred * inv_std, inv_std


def place():
    rank = lax.axis_index('tp')
    return rank // (SIDE * CORES), (rank // CORES) % SIDE, rank % CORES


def device(y, x, c):
    return {'tp': (((y + SIDE) % SIDE) * SIDE + (x + SIDE) % SIDE) * CORES + c}


def gather_kernel(h_ref, e_ref, gain_ref, bias_ref, code_ref, x_all, e_all, c_all, x_buf, send, recv, local):
    y, x, c = place()
    xp, xm, xo = device(y, x + 1, c), device(y, x - 1, c), device(y, x + 2, c)
    yp, ym, yo = device(y + 1, x, c), device(y - 1, x, c), device(y + 2, x, c)
    pc = device(y, x, 1 - c)
    barrier = pltpu.get_barrier_semaphore()
    peers = (xp, xm, xo, yp, ym, yo, pc)
    for peer in peers:
        pl.semaphore_signal(barrier, inc=1, device_id=peer, device_id_type=MESH)
    pl.semaphore_wait(barrier, len(peers))

    rows = h_ref.shape[0]
    lo, hi = pl.ds(0, rows // 2), pl.ds(rows // 2, rows // 2)

    def remote(i, src, dst, to):
        return pltpu.make_async_remote_copy(src_ref=src, dst_ref=dst, send_sem=send.at[i], recv_sem=recv.at[i], device_id=to, device_id_type=MESH)

    def ring(first, src, all_ref, unit, up, down):
        return [
            remote(first + 0, src.at[lo], all_ref.at[unit, lo], up),
            remote(first + 1, src.at[hi], all_ref.at[2 * unit, hi], down),
            remote(first + 2, src.at[hi], all_ref.at[unit, hi], up),
            remote(first + 3, src.at[lo], all_ref.at[2 * unit, lo], down),
            remote(first + 4, all_ref.at[unit, lo], all_ref.at[3 * unit, lo], up),
            remote(first + 5, all_ref.at[2 * unit, hi], all_ref.at[3 * unit, hi], down),
        ]

    xs = ring(0, x_all.at[0], x_all, 1, xp, xm)
    es = ring(6, e_ref, e_all, 2, yp, ym)
    swap = [
        remote(12, e_ref, e_all.at[1], pc),
        remote(13, e_all.at[2], e_all.at[3], pc),
        remote(14, e_all.at[4], e_all.at[5], pc),
        remote(15, e_all.at[6, lo], e_all.at[7, lo], pc),
        remote(16, e_all.at[6, hi], e_all.at[7, hi], pc),
    ]
    codes = [
        remote(17, code_ref, c_all.at[0, 0, 1], xp),
        remote(18, code_ref, c_all.at[0, 0, 2], xm),
        remote(19, code_ref, c_all.at[0, 0, 3], xo),
        remote(20, c_all.at[0, 0], c_all.at[0, 1], yp),
        remote(21, c_all.at[0, 0], c_all.at[0, 2], ym),
        remote(22, c_all.at[0, 0], c_all.at[0, 3], yo),
        remote(23, c_all.at[0], c_all.at[1], pc),
    ]
    keep_e = pltpu.make_async_copy(e_ref, e_all.at[0], local.at[0])
    keep_x = pltpu.make_async_copy(x_buf, x_all.at[0], local.at[1])
    keep_c = pltpu.make_async_copy(code_ref, c_all.at[0, 0, 0], local.at[2])

    for copy in es[:4] + swap[:1] + codes[:3] + [keep_e, keep_c]:
        copy.start()
    step = rows // 4

    def norm(i, carry):
        at = pl.ds(pl.multiple_of(i * step, step), step)
        x_hat, _ = normalize(h_ref[at, :])
        x_buf[at, :] = (x_hat * gain_ref[...] + bias_ref[...]).astype(x_buf.dtype)
        return carry

    lax.fori_loop(0, 4, norm, 0)
    keep_x.start()
    keep_x.wait()
    for copy in xs[:4]:
        copy.start()
    keep_c.wait()
    for copy in codes[:3]:
        copy.wait_recv()
    for copy in codes[3:6]:
        copy.start()
    es[0].wait_recv()
    es[4].start()
    es[1].wait_recv()
    es[5].start()
    xs[0].wait_recv()
    xs[4].start()
    xs[1].wait_recv()
    xs[5].start()
    es[2].wait_recv()
    swap[1].start()
    es[3].wait_recv()
    swap[2].start()
    for copy in codes[3:6]:
        copy.wait_recv()
    codes[6].start()
    es[4].wait_recv()
    swap[3].start()
    es[5].wait_recv()
    swap[4].start()
    for copy in xs[2:] + swap + codes[6:]:
        copy.wait_recv()
    for copy in xs + es + swap + codes:
        copy.wait_send()
    keep_e.wait()


def gather_call(hidden, embed, gain, bias, code):
    rows, dim = hidden.shape
    vmem, anywhere = pl.BlockSpec(memory_space=pltpu.VMEM), pl.BlockSpec(memory_space=pl.ANY)
    return pl.pallas_call(
        gather_kernel,
        out_shape=(
            jax.ShapeDtypeStruct((SIDE, rows, dim), jnp.bfloat16),
            jax.ShapeDtypeStruct((SIDE * CORES,) + embed.shape, jnp.bfloat16),
            jax.ShapeDtypeStruct((CORES, SIDE, SIDE) + code.shape, jnp.int32),
        ),
        in_specs=[vmem] * 5,
        out_specs=(anywhere,) * 3,
        scratch_shapes=[
            pltpu.VMEM((rows, dim), jnp.bfloat16),
            pltpu.SemaphoreType.DMA((24,)),
            pltpu.SemaphoreType.DMA((24,)),
            pltpu.SemaphoreType.DMA((3,)),
        ],
        compiler_params=pltpu.CompilerParams(collective_id=0, has_side_effects=True),
        cost_estimate=pl.CostEstimate(flops=10**10, bytes_accessed=10**7, transcendentals=0),
    )(hidden, embed, gain.reshape(1, dim), bias.reshape(1, dim), code)


def column_ids(col, vocab, y, x, c):
    block, within = col // vocab, col % vocab
    ring_at = block // CORES
    off = jnp.where(ring_at == 0, 0, jnp.where(ring_at == 1, SIDE - 1, ring_at - 1))
    core = (c + block % CORES) % CORES
    return ((((y + off) % SIDE) * SIDE + x) * CORES + core) * vocab + within


def logits_kernel(vocab, step, x_ref, e_ref, code_ref, ids_ref, z_ref, stat_ref):
    x = x_ref[...]
    tile = x.shape[0]
    code = code_ref[...]
    run_max = run_sum = run_tgt = None
    for at in range(0, e_ref.shape[0], step):
        z = lax.dot_general(x, e_ref[at:at + step, :], (((1,), (1,)), ((), ())), preferred_element_type=jnp.float32)
        z_ref[:, at:at + step] = z
        parts = [z[:, g:g + 128] for g in range(0, step, 128)]
        new_max = functools.reduce(jnp.maximum, parts if run_max is None else parts + [run_max])
        new_sum = functools.reduce(jnp.add, [jnp.exp(p - new_max) for p in parts])
        new_tgt = functools.reduce(jnp.add, [jnp.where(ids_ref[:, at + g:at + g + 128] == code, p, 0.0) for g, p in zip(range(0, step, 128), parts)])
        if run_max is not None:
            new_sum = new_sum + run_sum * jnp.exp(run_max - new_max)
            new_tgt = new_tgt + run_tgt
        run_max, run_sum, run_tgt = new_max, new_sum, new_tgt
    peak = jnp.max(run_max, axis=1, keepdims=True)
    norm = jnp.sum(run_sum * jnp.exp(run_max - peak), axis=1, keepdims=True)
    tgt = jnp.sum(run_tgt, axis=1, keepdims=True)
    lane = lax.broadcasted_iota(jnp.int32, (tile, 128), 1)
    stat = jnp.where(lane == 0, peak, jnp.where(lane == 1, norm, tgt))
    stat_ref[...] = stat.T[:8, :]


def logits_call(x, e, code, ids, vocab):
    (rows, dim), width = x.shape, e.shape[0]
    tile = rows // SIDE
    return pl.pallas_call(
        functools.partial(logits_kernel, vocab, 512),
        grid=(rows // tile,),
        out_shape=(jax.ShapeDtypeStruct((rows, width), jnp.float32), jax.ShapeDtypeStruct((8, rows), jnp.float32)),
        in_specs=[
            pl.BlockSpec((tile, dim), lambda i: (i, 0)),
            pl.BlockSpec((width, dim), lambda i: (0, 0), pipeline_mode=pl.Buffered(1)),
            pl.BlockSpec((tile, 1), lambda i: (i, 0)),
            pl.BlockSpec((1, width), lambda i: (0, 0)),
        ],
        out_specs=(pl.BlockSpec((tile, width), lambda i: (i, 0)), pl.BlockSpec((8, tile), lambda i: (0, i))),
        compiler_params=pltpu.CompilerParams(vmem_limit_bytes=VMEM_LIMIT),
        cost_estimate=pl.CostEstimate(flops=2 * rows * width * dim, bytes_accessed=rows * width * 4, transcendentals=rows * width),
    )(x, e, code, ids)


def lse_kernel(stat_ref, c_ref, code_ref, rows_ref, cols_ref, got, send, recv):
    y, x, c = place()
    shifts = (1, -1, 2)
    peers = [device(y, x + s, c) for s in shifts]
    barrier = pltpu.get_barrier_semaphore()
    for peer in peers:
        pl.semaphore_signal(barrier, inc=1, device_id=peer, device_id_type=MESH)
    pl.semaphore_wait(barrier, len(peers))
    copies = [
        pltpu.make_async_remote_copy(src_ref=stat_ref, dst_ref=got.at[i], send_sem=send.at[i], recv_sem=recv.at[i], device_id=peer, device_id_type=MESH)
        for i, peer in enumerate(peers)
    ]
    for copy in copies:
        copy.start()
    count = jnp.sum(jnp.sum((c_ref[...] >= 0).astype(jnp.float32), axis=0, keepdims=True), axis=1, keepdims=True)
    for copy in copies:
        copy.wait_recv()
    tokens = stat_ref.shape[1] // SIDE
    line = lax.broadcasted_iota(jnp.int32, (128, tokens), 0)
    where_of = {o % SIDE: k for k, o in enumerate(OFFSETS)}
    for k, off in enumerate(OFFSETS):
        views = [stat_ref[:, k * tokens:(k + 1) * tokens]]
        for i, s in enumerate(shifts):
            at = where_of[(off + s) % SIDE]
            views.append(got[i, :, at * tokens:(at + 1) * tokens])
        peak = functools.reduce(jnp.maximum, [v[0:1] for v in views])
        norm = functools.reduce(jnp.add, [v[1:2] * jnp.exp(v[0:1] - peak) for v in views])
        tgt = functools.reduce(jnp.add, [v[2:3] for v in views])
        code = code_ref[:, k * tokens:(k + 1) * tokens]
        weight = jnp.where(code >= 0, 1.0, 0.0)
        lse = peak + jnp.log(norm)
        cols = jnp.where(line == 0, lse, jnp.where(line == 1, weight / count, jnp.where(line == 2, code, 0.0)))
        cols_ref[k * tokens:(k + 1) * tokens, :] = cols.T
        line8 = line[:8]
        rows_ref[:, k * tokens:(k + 1) * tokens] = jnp.where(line8 == 0, (lse - tgt) * weight, jnp.where(line8 == 1, count, 0.0))
    for copy in copies:
        copy.wait_send()


def lse_call(stat, c_all, code_row):
    vmem = pl.BlockSpec(memory_space=pltpu.VMEM)
    return pl.pallas_call(
        lse_kernel,
        out_shape=(jax.ShapeDtypeStruct(stat.shape, jnp.float32), jax.ShapeDtypeStruct((stat.shape[1], 128), jnp.float32)),
        in_specs=[vmem] * 3,
        out_specs=(vmem, vmem),
        scratch_shapes=[pltpu.VMEM((3,) + stat.shape, jnp.float32), pltpu.SemaphoreType.DMA((3,)), pltpu.SemaphoreType.DMA((3,))],
        compiler_params=pltpu.CompilerParams(collective_id=1, has_side_effects=True),
        cost_estimate=pl.CostEstimate(flops=10**9, bytes_accessed=10**5, transcendentals=0),
    )(stat, c_all, code_row)


PHASES = (((3, 0), (3, 1)), ((2, 1), (1, 0)), ((2, 0), (1, 1)), ((0, 0), (0, 1)))


def backward_kernel(z_any, x_any, e_any, cols_ref, rows_ref, ids_ref, h_ref, gain_ref, dh_ref, sums_ref, de_any, xr, yr, dr, dz, xa, ea, xs, ys, ss, more, red, load, zsem, xsend, xrecv, ysend, yrecv, ssend, srecv, keep, rsend, rrecv):
    y, x, c = place()
    up = (device(y, x + 1, c), device(y + 1, x, c))
    down = (device(y, x - 1, c), device(y - 1, x, c))
    other = device(y, x, 1 - c)
    barrier = pltpu.get_barrier_semaphore()
    far = (device(y, x + 2, c), device(y + 2, x, c))
    for peer in up + down + far + (other,):
        pl.semaphore_signal(barrier, inc=1, device_id=peer, device_id_type=MESH)

    tokens, dim = h_ref.shape
    half = tokens // 2
    vocab = ea.shape[0] // (SIDE * CORES)
    wide = 512

    slots, span = ys.shape[0], 1024
    n_span = z_any.shape[1] // span
    per_block = 2 * n_span
    n_z = SIDE * per_block

    def spot(q):
        block, part = SIDE - 1 - q // per_block, (q // n_span) % 2
        return pl.multiple_of(block * tokens + part * half, half), pl.multiple_of((q % n_span) * span, span)

    def fetch(q):
        row, col = spot(q)
        return pltpu.make_async_copy(z_any.at[pl.ds(row, half), pl.ds(col, span)], ys.at[q % slots, :, pl.ds(0, span)], zsem.at[q % slots])

    loads = [pltpu.make_async_copy(e_any, ea, load.at[2]), pltpu.make_async_copy(x_any, xa, load.at[3])]
    for q in range(slots - 1):
        fetch(q).start()
    loads[0].start()

    def d_logits(q, carry):
        @pl.when(q + slots - 1 < n_z)
        def _():
            fetch(q + slots - 1).start()

        fetch(q).wait()
        row, col = spot(q)
        at = pl.ds(row, half)
        stat = cols_ref[at, :]
        lse, scale, code = stat[:, 0:1], stat[:, 1:2], stat[:, 2:3]
        for v in range(0, span, wide):
            here = pl.ds(pl.multiple_of(col + v, wide), wide)
            hot = jnp.where(ids_ref[:, here] == code, 1.0, 0.0)
            dz[at, here] = ((jnp.exp(ys[q % slots, :, v:v + wide] - lse) - hot) * scale).astype(dz.dtype)
        return carry

    lax.fori_loop(0, per_block, d_logits, 0)
    loads[1].start()
    pl.semaphore_wait(barrier, 7)

    def remote(src, dst, send, recv, to):
        return pltpu.make_async_remote_copy(src_ref=src, dst_ref=dst, send_sem=send, recv_sem=recv, device_id=to, device_id_type=MESH)

    xc, yc, sc = [], [], []
    for p in range(3):
        s = 2 * (p % 2)
        xc.append([remote(xs.at[s + j], xr.at[2 * p + j], xsend.at[2 * p + j], xrecv.at[2 * p + j], (up, down)[j][0]) for j in range(2)])
        yc.append([remote(ys.at[s + j], yr.at[2 * p + j], ysend.at[2 * p + j], yrecv.at[2 * p + j], (up, down)[j][1]) for j in range(2)])
    for p in range(4):
        sc.append([remote(ss.at[j], dr.at[2 * p + j], ssend.at[2 * p + j], srecv.at[2 * p + j], other) for j in range(2)])

    def add(dst, terms):
        for group in zip(*terms):
            copies = [pltpu.make_async_copy(ref, more.at[j], load.at[j]) for j, ref in enumerate(group)]
            for copy in copies:
                copy.start()
            for copy in copies:
                copy.wait()
            for j in range(2):
                dst[j][...] = dst[j][...] + more[j]

    def pick(j, pair):
        return jnp.where(j == 0, pair[0], pair[1])

    def x_tiles(p, s):
        at = [block * tokens + part * half for block, part in PHASES[p]]

        def tile(i, carry):
            j, n = i // (dim // wide), i % (dim // wide)
            r = pl.ds(pl.multiple_of(pick(j, at), half), half)
            cols = pl.ds(pl.multiple_of(n * wide, wide), wide)
            xs[s + j, :, cols] = lax.dot_general(dz[r, :], ea[:, cols], (((1,), (0,)), ((), ())), preferred_element_type=jnp.float32)
            return carry

        lax.fori_loop(0, 2 * (dim // wide), tile, 0)

    def y_tiles(p, core, out, s):
        part = vocab // 2
        at = [(block * CORES + core) * vocab + h * part for block, h in PHASES[p]]

        def tile(i, carry):
            j, n = i // (dim // wide), i % (dim // wide)
            r = pl.ds(pl.multiple_of(pick(j, at), part), part)
            cols = pl.ds(pl.multiple_of(n * wide, wide), wide)
            out[s + j, :, cols] = lax.dot_general(dz[:, r], xa[:, cols], (((0,), (0,)), ((), ())), preferred_element_type=jnp.float32)
            return carry

        lax.fori_loop(0, 2 * (dim // wide), tile, 0)

    loads[0].wait()
    for p in range(4):
        s = 2 * (p % 2)
        if p >= 2:
            for copy in xc[p - 2]:
                copy.wait_send()
        x_tiles(p, s)
        if p == 2:
            for copy in xc[0]:
                copy.wait_recv()
            add([xs.at[s], xs.at[s + 1]], [[xr.at[0]], [xr.at[1]]])
        if p < 3:
            for copy in xc[p]:
                copy.start()
        if p == 0:
            lax.fori_loop(per_block, n_z, d_logits, 0)
            loads[1].wait()
        if p >= 1:
            for copy in sc[p - 1]:
                copy.wait_send()
        y_tiles(p, 1, ss, 0)
        for copy in sc[p]:
            copy.start()
        if p >= 2:
            for copy in yc[p - 2]:
                copy.wait_send()
        y_tiles(p, 0, ys, s)
        for copy in sc[p]:
            copy.wait_recv()
        add([ys.at[s], ys.at[s + 1]], [[dr.at[2 * p]], [dr.at[2 * p + 1]]])
        if p == 2:
            for copy in yc[0]:
                copy.wait_recv()
            add([ys.at[s], ys.at[s + 1]], [[yr.at[0]], [yr.at[1]]])
        if p < 3:
            for copy in yc[p]:
                copy.start()

    for copy in xc[1] + xc[2]:
        copy.wait_recv()
    add([xs.at[2], xs.at[3]], [[xr.at[4], xr.at[3]], [xr.at[2], xr.at[5]]])
    step = half // 4
    sums_ref[...] = jnp.zeros(sums_ref.shape, jnp.float32)

    def norm_back(i, carry):
        j, r = i // 4, i % 4
        at = pl.ds(pl.multiple_of(i * step, step), step)
        d_normed = xs[2 + j, pl.ds(pl.multiple_of(r * step, step), step), :]
        x_hat, inv_std = normalize(h_ref[at, :])
        g = d_normed * gain_ref[...]
        centre = jnp.mean(g, axis=-1, keepdims=True)
        proj = jnp.mean(g * x_hat, axis=-1, keepdims=True)
        dh_ref[at, :] = (inv_std * (g - centre - x_hat * proj)).astype(dh_ref.dtype)
        sums_ref[0:1, :] += jnp.sum(d_normed * x_hat, axis=0, keepdims=True)
        sums_ref[1:2, :] += jnp.sum(d_normed, axis=0, keepdims=True)
        return carry

    lax.fori_loop(0, 8, norm_back, 0)
    sums_ref[2:3, 0:128] = functools.reduce(jnp.add, [rows_ref[0:1, g:g + 128] for g in range(0, tokens, 128)])

    stages = ((x, [device(y, x + d, c) for d in (1, -1, 2)]), (y, [device(y + d, x, c) for d in (1, -1, 2)]), (c, [other]))
    k = 0
    for stage, (pos, peers) in enumerate(stages):
        red[stage, pos] = sums_ref[...]
        copies = []
        for peer in peers:
            copies.append(remote(red.at[stage, pos], red.at[stage, pos], rsend.at[k], rrecv.at[k], peer))
            k += 1
        for copy in copies:
            copy.start()
        for copy in copies:
            copy.wait_recv()
        sums_ref[...] = functools.reduce(jnp.add, [red[stage, i] for i in range(len(peers) + 1)])
        for copy in copies:
            copy.wait_send()

    for copy in yc[1] + yc[2]:
        copy.wait_recv()
    add([ys.at[2], ys.at[3]], [[yr.at[4], yr.at[3]], [yr.at[2], yr.at[5]]])
    outs = [pltpu.make_async_copy(ys.at[2 + j], de_any.at[pl.ds(j * (vocab // 2), vocab // 2)], keep.at[j]) for j in range(2)]
    for copy in outs:
        copy.start()
    for copy in outs:
        copy.wait()
    for copy in xc[2] + yc[2] + sc[3]:
        copy.wait_send()


def backward_call(z, x, e, cols, rows, ids, hidden, gain):
    tokens, dim = hidden.shape
    vocab = e.shape[0] // (SIDE * CORES)
    vmem, anywhere = pl.BlockSpec(memory_space=pltpu.VMEM), pl.BlockSpec(memory_space=pl.ANY)
    f32, tile = jnp.float32, (tokens // 2, dim)
    sem = pltpu.SemaphoreType.DMA
    out = pl.pallas_call(
        backward_kernel,
        out_shape=(
            jax.ShapeDtypeStruct(hidden.shape, jnp.bfloat16),
            jax.ShapeDtypeStruct((8, dim), f32),
            jax.ShapeDtypeStruct((vocab, dim), f32),
            jax.ShapeDtypeStruct((6,) + tile, f32),
            jax.ShapeDtypeStruct((6,) + tile, f32),
            jax.ShapeDtypeStruct((8,) + tile, f32),
        ),
        in_specs=[anywhere] * 3 + [vmem] * 5,
        out_specs=(vmem, vmem) + (anywhere,) * 4,
        scratch_shapes=[
            pltpu.VMEM(z.shape, jnp.bfloat16),
            pltpu.VMEM(x.shape, x.dtype),
            pltpu.VMEM(e.shape, e.dtype),
            pltpu.VMEM((4,) + tile, f32),
            pltpu.VMEM((4,) + tile, f32),
            pltpu.VMEM((2,) + tile, f32),
            pltpu.VMEM((2,) + tile, f32),
            pltpu.VMEM((3, SIDE, 8, dim), f32),
            sem((4,)), sem((4,)), sem((6,)), sem((6,)), sem((6,)), sem((6,)), sem((8,)), sem((8,)), sem((2,)), sem((7,)), sem((7,)),
        ],
        compiler_params=pltpu.CompilerParams(collective_id=2, has_side_effects=True, vmem_limit_bytes=67043328),
        cost_estimate=pl.CostEstimate(flops=4 * z.size * dim, bytes_accessed=10**8, transcendentals=0),
    )(z, x, e, cols, rows, ids, hidden, gain.reshape(1, dim))
    return out[:3]


def solution(mesh):
    group = mesh.shape['tp']
    assert group == SIDE * SIDE * CORES

    def body(hidden, ln_gain, ln_bias, embed, targets, loss_mask):
        tokens, dim = hidden.shape
        vocab = embed.shape[0]
        rank = lax.axis_index('tp')
        y, x, c = rank // (SIDE * CORES), (rank // CORES) % SIDE, rank % CORES
        f32 = jnp.float32

        code = jnp.where(loss_mask > 0, targets, -1)
        code = jnp.pad(code.reshape(-1, 128), ((0, 8 - tokens // 128), (0, 0)), constant_values=-1)
        x_all, e_all, c_all = gather_call(hidden, embed, ln_gain, ln_bias, code)
        n_all, v_all = SIDE * tokens, SIDE * CORES * vocab
        x_all, e_all = x_all.reshape(n_all, dim), e_all.reshape(v_all, dim)
        codes = c_all[0, 0, :, :tokens // 128].reshape(n_all)
        code_col = codes[:, None]
        ids = column_ids(lax.broadcasted_iota(jnp.int32, (1, v_all), 1), vocab, y, x, c)
        logits, stat = logits_call(x_all, e_all, code_col, ids, vocab)
        rows, cols = lse_call(stat, c_all.reshape(-1, 128), codes.astype(f32).reshape(1, n_all))
        own_loss = rows[0, :tokens]
        d_hidden, sums, d_embed = backward_call(logits, x_all, e_all, cols, rows, ids.astype(f32), hidden, ln_gain)
        mean_loss = (jnp.sum(sums[2, :128]) / rows[1, 0]).reshape(1)
        return own_loss, mean_loss, d_hidden, d_embed, sums[0], sums[1]

    token_rows = P(('dp', 'tp'))
    token_mat = P(('dp', 'tp'), None)
    return jax.shard_map(body, mesh=mesh, in_specs=(token_mat, P(), P(), P('tp', None), token_rows, token_rows), out_specs=(token_rows, P('dp'), token_mat, token_mat, P('dp'), P('dp')), check_vma=False)
```

```python
import functools

import jax
import jax.numpy as jnp
from jax import lax
from jax.experimental import pallas as pl
from jax.experimental.pallas import tpu as pltpu
from jax.sharding import PartitionSpec as P

LN_EPS = 1e-5
CORES = 2
SIDE = 4
OFFSETS = (0, -1, 1, 2)
VMEM_LIMIT = 67043328
MESH = pl.DeviceIdType.MESH
BOTH = (0, 1)
LANES = 128


def row_sum(v):
    return jnp.sum(v, axis=1, keepdims=True)


def row_mean(v):
    return jnp.mean(v, axis=-1, keepdims=True)


def col_sum(v):
    return jnp.sum(v, axis=0, keepdims=True)


def dot(a, b, of_a, of_b):
    return lax.dot_general(a, b, (((of_a,), (of_b,)), ((), ())), preferred_element_type=jnp.float32)


def normalize(hidden):
    h_f32 = hidden.astype(jnp.float32)
    centred = h_f32 - row_mean(h_f32)
    inv_std = lax.rsqrt(row_mean(centred * centred) + LN_EPS)
    return centred * inv_std, inv_std


def place():
    rank = lax.axis_index('tp')
    return rank // (SIDE * CORES), (rank // CORES) % SIDE, rank % CORES


def device(y, x, c):
    return {'tp': (((y + SIDE) % SIDE) * SIDE + (x + SIDE) % SIDE) * CORES + c}


def column_ids(col, vocab, y, x, c):
    block, within = col // vocab, col % vocab
    ring_at = block // CORES
    off = jnp.where(ring_at == 0, 0, jnp.where(ring_at == 1, SIDE - 1, ring_at - 1))
    core = (c + block % CORES) % CORES
    return ((((y + off) % SIDE) * SIDE + x) * CORES + core) * vocab + within


PHASES = (((3, 0), (3, 1)), ((2, 1), (1, 0)), ((2, 0), (1, 1)), ((0, 0), (0, 1)))


def step_kernel(
    h_ref, e_any, affine_ref, code_any, ids_ref,
    dh_ref, sums_ref, rows_ref, de_any, z_any, xr, yr, dr,
    dz, xa, ea, xs, ys, ss, more, red, cols_ref, c_all, got, stat_ref,
    load, zsem, gsend, grecv, lsend, lrecv, xsend, xrecv, ysend, yrecv, ssend, srecv, keep, rsend, rrecv, osend, orecv,
):
    y, x, c = place()
    up = (device(y, x + 1, c), device(y + 1, x, c))
    down = (device(y, x - 1, c), device(y - 1, x, c))
    opposite = (device(y, x + 2, c), device(y + 2, x, c))
    other = device(y, x, 1 - c)
    barrier = pltpu.get_barrier_semaphore()
    for peer in up + down + opposite + (other,):
        pl.semaphore_signal(barrier, inc=1, device_id=peer, device_id_type=MESH)

    tokens, dim = h_ref.shape
    half = tokens // 2
    vocab = ea.shape[0] // (SIDE * CORES)
    wide = 512
    f32 = jnp.float32
    slots, span = ys.shape[0], CORES * vocab

    def remote(src, dst, send, recv, to):
        return pltpu.make_async_remote_copy(src_ref=src, dst_ref=dst, send_sem=send, recv_sem=recv, device_id=to, device_id_type=MESH)

    def xat(block, part=None):
        return xa.at[pl.ds(block * tokens, tokens)] if part is None else xa.at[pl.ds(block * tokens + part * half, half)]

    def eat(block, part=None):
        return ea.at[pl.ds(block * vocab, vocab)] if part is None else ea.at[pl.ds(block * vocab + part * (vocab // 2), vocab // 2)]

    def e_own(part):
        return e_any.at[pl.ds(part * (vocab // 2), vocab // 2)]

    tags = iter(range(gsend.shape[0]))

    def moving(src, dst, to):
        tag = next(tags)
        return remote(src, dst, gsend.at[tag], grecv.at[tag], to)

    def ring(own, at, unit, to_up, to_down):
        return [
            moving(own(0), at(unit, 0), to_up),
            moving(own(1), at(2 * unit, 1), to_down),
            moving(own(1), at(unit, 1), to_up),
            moving(own(0), at(2 * unit, 0), to_down),
            moving(at(unit, 0), at(3 * unit, 0), to_up),
            moving(at(2 * unit, 1), at(3 * unit, 1), to_down),
        ]

    gx = ring(lambda part: xat(0, part), xat, 1, up[0], down[0])
    ge = ring(e_own, eat, 2, up[1], down[1])
    swap = [
        moving(e_any, eat(1), other),
        moving(eat(2), eat(3), other),
        moving(eat(4), eat(5), other),
        moving(eat(6, 0), eat(7, 0), other),
        moving(eat(6, 1), eat(7, 1), other),
    ]
    codes = [
        moving(code_any, c_all.at[0, 0, 1], up[0]),
        moving(code_any, c_all.at[0, 0, 2], down[0]),
        moving(code_any, c_all.at[0, 0, 3], opposite[0]),
        moving(c_all.at[0, 0], c_all.at[0, 1], up[1]),
        moving(c_all.at[0, 0], c_all.at[0, 2], down[1]),
        moving(c_all.at[0, 0], c_all.at[0, 3], opposite[1]),
        moving(c_all.at[0], c_all.at[1], other),
    ]
    keep_e = pltpu.make_async_copy(e_any, eat(0), load.at[0])
    keep_c = pltpu.make_async_copy(code_any, c_all.at[0, 0, 0], load.at[1])
    keep_e.start()
    keep_c.start()
    pl.semaphore_wait(barrier, 7)
    for copy in ge[:4] + swap[:1] + codes[:3]:
        copy.start()
    step = half // 4

    def norm(i, carry):
        at = pl.ds(pl.multiple_of(i * step, step), step)
        x_hat, _ = normalize(h_ref[at, :])
        xa[at, :] = (x_hat * affine_ref[0:1, :] + affine_ref[1:2, :]).astype(xa.dtype)
        return carry

    lax.fori_loop(0, 8, norm, 0)

    halves = 2 * SIDE
    for slot in range(2):
        for hb in range(halves // 2):
            for kind, value in enumerate((-jnp.inf, 0.0, 0.0)):
                lane = (3 * hb + kind) * LANES
                ss[slot, :, lane:lane + LANES] = jnp.full((half, LANES), value, f32)
    for copy in gx[:4]:
        copy.start()
    keep_c.wait()
    for copy in codes[:3]:
        copy.wait_recv()
    for copy in codes[3:6]:
        copy.start()

    for block in range(SIDE):
        for r in range(tokens // LANES):
            hb, at = (block * tokens + r * LANES) // half, (r * LANES) % half
            more[0, at:at + LANES, hb * LANES:(hb + 1) * LANES] = jnp.broadcast_to(c_all[0, 0, block, r:r + 1, :].astype(f32), (LANES, LANES)).T

    def z_out(u, b, k, j):
        rows = pl.ds(pl.multiple_of(b * tokens + j * half, half), half)
        cols = pl.ds(pl.multiple_of(k * span, span), span)
        s = (2 * u) % slots + j
        return pltpu.make_async_copy(ys.at[s, :, pl.ds(0, span)], z_any.at[rows, cols], zsem.at[s])

    def logits(u, b, k):
        @pl.when(u >= 2)
        def _():
            for j in BOTH:
                z_out(u, b, k, j).wait()

        at = pl.ds(pl.multiple_of(b * tokens, tokens), tokens)
        s = (2 * u) % slots
        for n in range(span // wide):
            ids_at = pl.ds(pl.multiple_of(k * span + n * wide, wide), wide)
            e_at = pl.ds(pl.multiple_of(k * span + n * wide, wide), wide)
            z = dot(xa[at, :], ea[e_at, :], 1, 1)
            ids = ids_ref[:, ids_at]
            for j in BOTH:
                zj = z[j * half:(j + 1) * half]
                ys[s + j, :, n * wide:(n + 1) * wide] = zj
                hb = 2 * b + j
                slot, lane = hb // SIDE, (hb % SIDE) * 3 * LANES
                lanes = [pl.ds(pl.multiple_of(lane + kind * LANES, LANES), LANES) for kind in range(3)]
                code = more[0, :, pl.ds(pl.multiple_of(hb * LANES, LANES), LANES)]
                old_max = ss[slot, :, lanes[0]]
                parts = [zj[:, g:g + LANES] for g in range(0, wide, LANES)]
                new_max = functools.reduce(jnp.maximum, parts + [old_max])
                new_sum = ss[slot, :, lanes[1]] * jnp.exp(old_max - new_max)
                ss[slot, :, lanes[1]] = functools.reduce(jnp.add, [new_sum] + [jnp.exp(part - new_max) for part in parts])
                hits = [jnp.where(ids[:, g:g + LANES] == code, part, 0.0) for g, part in zip(range(0, wide, LANES), parts)]
                ss[slot, :, lanes[2]] = functools.reduce(jnp.add, [ss[slot, :, lanes[2]]] + hits)
                ss[slot, :, lanes[0]] = new_max
        for j in BOTH:
            z_out(u, b, k, j).start()

    keep_e.wait()
    swap[0].wait_recv()
    logits(0, 0, 0)
    ge[0].wait_recv()
    ge[4].start()
    ge[1].wait_recv()
    ge[5].start()
    gx[0].wait_recv()
    gx[4].start()
    gx[1].wait_recv()
    gx[5].start()
    ge[2].wait_recv()
    swap[1].start()
    ge[3].wait_recv()
    swap[2].start()
    for copy in codes[3:6]:
        copy.wait_recv()
    codes[6].start()
    for copy in gx[2:4] + swap[1:3]:
        copy.wait_recv()

    def near(u, carry):
        logits(u, u // 3, u % 3)
        return carry

    lax.fori_loop(1, 8, near, 0)
    ge[4].wait_recv()
    swap[3].start()
    ge[5].wait_recv()
    swap[4].start()
    lax.fori_loop(8, 9, near, 0)
    gx[4].wait_recv()
    gx[5].wait_recv()

    def far_tokens(u, carry):
        logits(u, SIDE - 1, u - 9)
        return carry

    lax.fori_loop(9, 12, far_tokens, 0)
    swap[3].wait_recv()
    swap[4].wait_recv()

    def far_vocab(u, carry):
        logits(u, u - 12, SIDE - 1)
        return carry

    lax.fori_loop(12, 16, far_vocab, 0)
    codes[6].wait_recv()

    for hb in range(halves):
        lanes = [slice((3 * (hb % SIDE) + kind) * LANES, (3 * (hb % SIDE) + kind + 1) * LANES) for kind in range(3)]
        run_max, run_sum, run_tgt = (ss[hb // SIDE, :, lane] for lane in lanes)
        peak = jnp.max(run_max, axis=1, keepdims=True)
        norm_sum = row_sum(run_sum * jnp.exp(run_max - peak))
        tgt = row_sum(run_tgt)
        lane = lax.broadcasted_iota(jnp.int32, (half, LANES), 1)
        stat_ref[:, hb * half:(hb + 1) * half] = jnp.where(lane == 0, peak, jnp.where(lane == 1, norm_sum, tgt)).T[:8, :]
    shifts = (1, -1, 2)
    stats = [remote(stat_ref, got.at[i], lsend.at[i], lrecv.at[i], peer) for i, peer in enumerate((up[0], down[0], opposite[0]))]
    for copy in stats:
        copy.start()
    count = row_sum(col_sum((c_all[...].reshape(-1, LANES) >= 0).astype(f32)))
    for j in BOTH:
        z_out(14, 0, 0, j).wait()
        z_out(15, 0, 0, j).wait()
    for copy in gx + ge + swap + codes:
        copy.wait_send()
    for copy in stats:
        copy.wait_recv()
    line = lax.broadcasted_iota(jnp.int32, (LANES, half), 0)
    where_of = {o % SIDE: k for k, o in enumerate(OFFSETS)}
    for hb in range(halves):
        block, part = hb // 2, hb % 2
        views = [stat_ref[:, hb * half:(hb + 1) * half]]
        for i, shift in enumerate(shifts):
            at = (2 * where_of[(OFFSETS[block] + shift) % SIDE] + part) * half
            views.append(got[i, :, at:at + half])
        peak = functools.reduce(jnp.maximum, [v[0:1] for v in views])
        norm_sum = functools.reduce(jnp.add, [v[1:2] * jnp.exp(v[0:1] - peak) for v in views])
        tgt = functools.reduce(jnp.add, [v[2:3] for v in views])
        lse = peak + jnp.log(norm_sum)
        cols_ref[hb * half:(hb + 1) * half, :] = jnp.where(line == 0, lse, 0.0).T
        code = more[0, :, hb * LANES:(hb + 1) * LANES]
        lane = lax.broadcasted_iota(jnp.int32, (half, LANES), 1)
        weight = jnp.where(code >= 0, 1.0, 0.0)
        rest = jnp.where(lane == 1, weight / count, jnp.where(lane == 2, code, 0.0))
        cols_ref[hb * half:(hb + 1) * half, :] += rest
        if block == 0:
            weight_row = jnp.where(lane == 0, weight, 0.0).T[0:1, :]
            line8 = line[:8]
            rows_ref[:, part * half:(part + 1) * half] = jnp.where(line8 == 0, (lse - tgt) * weight_row, jnp.where(line8 == 1, count, 0.0))
    for copy in stats:
        copy.wait_send()

    n_span = z_any.shape[1] // span
    per_block = 2 * n_span
    n_z = SIDE * per_block

    def spot(q):
        block, part = SIDE - 1 - q // per_block, (q // n_span) % 2
        return pl.multiple_of(block * tokens + part * half, half), pl.multiple_of((q % n_span) * span, span)

    def fetch(q):
        row, col = spot(q)
        return pltpu.make_async_copy(z_any.at[pl.ds(row, half), pl.ds(col, span)], ys.at[q % slots, :, pl.ds(0, span)], zsem.at[q % slots])

    for q in range(slots - 1):
        fetch(q).start()

    def d_logits(q, carry):
        @pl.when(q + slots - 1 < n_z)
        def _():
            fetch(q + slots - 1).start()

        fetch(q).wait()
        row, col = spot(q)
        at = pl.ds(row, half)
        stat = cols_ref[at, :]
        lse, scale, code = (stat[:, k:k + 1] for k in range(3))
        for v in range(0, span, wide):
            here = pl.ds(pl.multiple_of(col + v, wide), wide)
            hot = jnp.where(ids_ref[:, here] == code, 1.0, 0.0)
            dz[at, here] = ((jnp.exp(ys[q % slots, :, v:v + wide] - lse) - hot) * scale).astype(dz.dtype)
        return carry

    lax.fori_loop(0, per_block, d_logits, 0)
    chunks = dim // wide

    def part_of(n):
        return pl.ds(pl.multiple_of(n * wide, wide), wide)

    def opening(kind, j, n):
        src, dst, to = ((xs, xr, (up, down)[j][0]), (ys, yr, (up, down)[j][1]), (ss, dr, other))[kind]
        tag = (kind * len(BOTH) + j) * chunks + n
        return remote(src.at[j, :, part_of(n)], dst.at[j, :, part_of(n)], osend.at[tag], orecv.at[tag], to)

    xc, yc, sc = ([[opening(kind, j, n) for n in range(chunks) for j in BOTH]] for kind in range(3))
    for p in range(1, SIDE):
        s = 2 * (p % 2)
        if p < SIDE - 1:
            xc.append([remote(xs.at[s + j], xr.at[2 * p + j], xsend.at[2 * p + j], xrecv.at[2 * p + j], (up, down)[j][0]) for j in BOTH])
            yc.append([remote(ys.at[s + j], yr.at[2 * p + j], ysend.at[2 * p + j], yrecv.at[2 * p + j], (up, down)[j][1]) for j in BOTH])
        sc.append([remote(ss.at[j], dr.at[2 * p + j], ssend.at[2 * p + j], srecv.at[2 * p + j], other) for j in BOTH])

    def two(ref, first):
        return [ref.at[first], ref.at[first + 1]]

    def add(dst, terms):
        copies = [pltpu.make_async_copy(ref, more.at[j], load.at[j]) for j, ref in enumerate(terms)]
        for copy in copies:
            copy.start()
        for copy in copies:
            copy.wait()
        for j in BOTH:
            dst[j][...] = dst[j][...] + more[j]

    def pick(j, pair):
        return jnp.where(j == 0, pair[0], pair[1])

    def x_tiles(p, s, first, last):
        at = [block * tokens + part * half for block, part in PHASES[p]]

        def tile(i, carry):
            j, n = i % 2, i // 2
            r = pl.ds(pl.multiple_of(pick(j, at), half), half)
            xs[s + j, :, part_of(n)] = dot(dz[r, :], ea[:, part_of(n)], 1, 0)
            return carry

        lax.fori_loop(2 * first, 2 * last, tile, 0)

    def y_tiles(p, core, out, s, first, last):
        part = vocab // 2
        at = [(block * CORES + core) * vocab + h * part for block, h in PHASES[p]]

        def tile(i, carry):
            j, n = i % 2, i // 2
            r = pl.ds(pl.multiple_of(pick(j, at), part), part)
            out[s + j, :, part_of(n)] = dot(dz[:, r], xa[:, part_of(n)], 0, 0)
            return carry

        lax.fori_loop(2 * first, 2 * last, tile, 0)

    def open_links(n, carry):
        x_tiles(0, 0, n, n + 1)
        for j in BOTH:
            opening(0, j, n).start()

        @pl.when(n == 0)
        def _():
            lax.fori_loop(per_block, n_z, d_logits, 0)

        y_tiles(0, 1, ss, 0, n, n + 1)
        for j in BOTH:
            opening(2, j, n).start()
        y_tiles(0, 0, ys, 0, n, n + 1)
        for j in BOTH:
            opening(2, j, n).wait_recv()
        copies = [pltpu.make_async_copy(dr.at[j, :, part_of(n)], more.at[j, :, part_of(n)], load.at[j]) for j in BOTH]
        for copy in copies:
            copy.start()
        for copy in copies:
            copy.wait()
        for j in BOTH:
            ys[j, :, part_of(n)] = ys[j, :, part_of(n)] + more[j, :, part_of(n)]
            opening(1, j, n).start()
        return carry

    lax.fori_loop(0, chunks, open_links, 0)
    for p in range(1, SIDE):
        s = 2 * (p % 2)
        if p >= 2:
            for copy in xc[p - 2]:
                copy.wait_send()
        x_tiles(p, s, 0, chunks)
        if p == 2:
            for copy in xc[0]:
                copy.wait_recv()
            add(two(xs, s), two(xr, 0))
        if p < 3:
            for copy in xc[p]:
                copy.start()
        for copy in sc[p - 1]:
            copy.wait_send()
        y_tiles(p, 1, ss, 0, 0, chunks)
        for copy in sc[p]:
            copy.start()
        if p >= 2:
            for copy in yc[p - 2]:
                copy.wait_send()
        y_tiles(p, 0, ys, s, 0, chunks)
        for copy in sc[p]:
            copy.wait_recv()
        add(two(ys, s), two(dr, 2 * p))
        if p == 2:
            for copy in yc[0]:
                copy.wait_recv()
            add(two(ys, s), two(yr, 0))
        if p < 3:
            for copy in yc[p]:
                copy.start()

    own_x, own_y = two(xs, 2), two(ys, 2)
    for own, landed, copies in ((own_x, xr, xc[1]), (own_y, yr, yc[1])):
        for copy in copies:
            copy.wait_recv()
        add(own, [landed.at[3], landed.at[2]])
    for copy in xc[2]:
        copy.wait_recv()
    add(own_x, two(xr, 4))
    step = half // 4
    sums_ref[...] = jnp.zeros(sums_ref.shape, jnp.float32)

    def norm_back(i, carry):
        j, r = i // 4, i % 4
        at = pl.ds(pl.multiple_of(i * step, step), step)
        d_normed = xs[2 + j, pl.ds(pl.multiple_of(r * step, step), step), :]
        x_hat, inv_std = normalize(h_ref[at, :])
        g = d_normed * affine_ref[0:1, :]
        centre, proj = row_mean(g), row_mean(g * x_hat)
        dh_ref[at, :] = (inv_std * (g - centre - x_hat * proj)).astype(dh_ref.dtype)
        sums_ref[0:1, :] += col_sum(d_normed * x_hat)
        sums_ref[1:2, :] += col_sum(d_normed)
        return carry

    lax.fori_loop(0, 8, norm_back, 0)
    sums_ref[2:3, 0:LANES] = functools.reduce(jnp.add, [rows_ref[0:1, g:g + LANES] for g in range(0, tokens, LANES)])

    stages = ((x, [device(y, x + d, c) for d in (1, -1, 2)]), (y, [device(y + d, x, c) for d in (1, -1, 2)]), (c, [other]))
    k = 0
    for stage, (pos, peers) in enumerate(stages):
        red[stage, pos] = sums_ref[...]
        copies = []
        for peer in peers:
            copies.append(remote(red.at[stage, pos], red.at[stage, pos], rsend.at[k], rrecv.at[k], peer))
            k += 1
        for copy in copies:
            copy.start()
        for copy in copies:
            copy.wait_recv()
        sums_ref[...] = functools.reduce(jnp.add, [red[stage, i] for i in range(len(peers) + 1)])
        for copy in copies:
            copy.wait_send()

    sums_ref[3:4, :] = jnp.broadcast_to(row_sum(sums_ref[2:3, 0:LANES]) / rows_ref[1:2, 0:1], (1, dim))

    for copy in yc[2]:
        copy.wait_recv()
    add(own_y, two(yr, 4))
    outs = [pltpu.make_async_copy(ys.at[2 + j], de_any.at[pl.ds(j * (vocab // 2), vocab // 2)], keep.at[j]) for j in BOTH]
    for copy in outs:
        copy.start()
    for copy in outs:
        copy.wait()
    for copy in xc[2] + yc[2] + sc[3]:
        copy.wait_send()


def step_call(hidden, embed, affine, code, ids):
    tokens, dim = hidden.shape
    vocab = embed.shape[0]
    n_tok, n_voc = SIDE * tokens, SIDE * CORES * vocab
    vmem, anywhere = pl.BlockSpec(memory_space=pltpu.VMEM), pl.BlockSpec(memory_space=pl.ANY)
    f32, bf16, tile = jnp.float32, jnp.bfloat16, (tokens // 2, dim)
    out = pl.pallas_call(
        step_kernel,
        out_shape=(
            jax.ShapeDtypeStruct(hidden.shape, bf16),
            jax.ShapeDtypeStruct((8, dim), f32),
            jax.ShapeDtypeStruct((8, tokens), f32),
            jax.ShapeDtypeStruct((vocab, dim), f32),
            jax.ShapeDtypeStruct((n_tok, n_voc), f32),
            jax.ShapeDtypeStruct((6,) + tile, f32),
            jax.ShapeDtypeStruct((6,) + tile, f32),
            jax.ShapeDtypeStruct((8,) + tile, f32),
        ),
        in_specs=[vmem, anywhere, vmem, anywhere, vmem],
        out_specs=(vmem, vmem, vmem) + (anywhere,) * 5,
        scratch_shapes=[
            pltpu.VMEM((n_tok, n_voc), bf16),
            pltpu.VMEM((n_tok, dim), bf16),
            pltpu.VMEM((n_voc, dim), bf16),
            pltpu.VMEM((4,) + tile, f32),
            pltpu.VMEM((4,) + tile, f32),
            pltpu.VMEM((2,) + tile, f32),
            pltpu.VMEM((2,) + tile, f32),
            pltpu.VMEM((3, SIDE, 8, dim), f32),
            pltpu.VMEM((n_tok, LANES), f32),
            pltpu.VMEM((CORES, SIDE, SIDE) + code.shape, jnp.int32),
            pltpu.VMEM((3, 8, n_tok), f32),
            pltpu.VMEM((8, n_tok), f32),
        ] + [pltpu.SemaphoreType.DMA((n,)) for n in (SIDE, SIDE, 24, 24, SIDE, SIDE) + (6,) * SIDE + (8,) * 5 + (18, 18)],
        compiler_params=pltpu.CompilerParams(collective_id=0, has_side_effects=True, vmem_limit_bytes=VMEM_LIMIT),
        cost_estimate=pl.CostEstimate(flops=6 * n_tok * n_voc * dim, bytes_accessed=10**8, transcendentals=2 * n_tok * n_voc),
    )(hidden, embed, affine, code, ids)
    return out[:4]


def solution(mesh):
    group = mesh.shape['tp']
    assert group == SIDE * SIDE * CORES

    def body(hidden, ln_gain, ln_bias, embed, targets, loss_mask):
        tokens, dim = hidden.shape
        vocab = embed.shape[0]
        rank = lax.axis_index('tp')
        y, x, c = rank // (SIDE * CORES), (rank // CORES) % SIDE, rank % CORES
        f32 = jnp.float32

        code = jnp.where(loss_mask > 0, targets, -1)
        code = jnp.pad(code.reshape(-1, LANES), ((0, 8 - tokens // LANES), (0, 0)), constant_values=-1)
        ids = column_ids(lax.broadcasted_iota(jnp.int32, (1, SIDE * CORES * vocab), 1), vocab, y, x, c).astype(f32)
        d_hidden, sums, rows, d_embed = step_call(hidden, embed, jnp.stack([ln_gain, ln_bias]), code, ids)
        own_loss = rows[0]
        return own_loss, sums[3, :1], d_hidden, d_embed, sums[0], sums[1]

    token_rows = P(('dp', 'tp'))
    token_mat = P(('dp', 'tp'), None)
    return jax.shard_map(body, mesh=mesh, in_specs=(token_mat, P(), P(), P('tp', None), token_rows, token_rows), out_specs=(token_rows, P('dp'), token_mat, token_mat, P('dp'), P('dp')), check_vma=False)
```

```python
import functools

import jax
import jax.numpy as jnp
from jax import lax
from jax.experimental import pallas as pl
from jax.experimental.pallas import tpu as pltpu
from jax.sharding import PartitionSpec as P

LN_EPS = 1e-5
CORES = 2
SIDE = 4
OFFSETS = (0, -1, 1, 2)
VMEM_LIMIT = 67043328
MESH = pl.DeviceIdType.MESH
BOTH = (0, 1)
LANES = 128


def row_sum(v):
    return jnp.sum(v, axis=1, keepdims=True)


def row_mean(v):
    return jnp.mean(v, axis=-1, keepdims=True)


def col_sum(v):
    return jnp.sum(v, axis=0, keepdims=True)


def dot(a, b, of_a, of_b):
    return lax.dot_general(a, b, (((of_a,), (of_b,)), ((), ())), preferred_element_type=jnp.float32)


def normalize(hidden):
    h_f32 = hidden.astype(jnp.float32)
    centred = h_f32 - row_mean(h_f32)
    inv_std = lax.rsqrt(row_mean(centred * centred) + LN_EPS)
    return centred * inv_std, inv_std


def place():
    rank = lax.axis_index('tp')
    return rank // (SIDE * CORES), (rank // CORES) % SIDE, rank % CORES


def device(y, x, c):
    return {'tp': (((y + SIDE) % SIDE) * SIDE + (x + SIDE) % SIDE) * CORES + c}


def column_ids(col, vocab, y, x, c):
    block, within = col // vocab, col % vocab
    ring_at = block // CORES
    off = jnp.where(ring_at == 0, 0, jnp.where(ring_at == 1, SIDE - 1, ring_at - 1))
    core = (c + block % CORES) % CORES
    return ((((y + off) % SIDE) * SIDE + x) * CORES + core) * vocab + within


PHASES = (((3, 0), (3, 1)), ((2, 1), (1, 0)), ((2, 0), (1, 1)), ((0, 0), (0, 1)))


def step_kernel(
    h_ref, e_any, affine_ref, code_any, ids_ref,
    dh_ref, sums_ref, rows_ref, de_any, z_any, xr, yr, dr,
    dz, xa, ea, xs, ys, ss, more, red, cols_ref, c_all, got, stat_ref,
    load, zsem, gsend, grecv, lsend, lrecv, xsend, xrecv, ysend, yrecv, ssend, srecv, keep, rsend, rrecv, osend, orecv,
):
    y, x, c = place()
    up = (device(y, x + 1, c), device(y + 1, x, c))
    down = (device(y, x - 1, c), device(y - 1, x, c))
    opposite = (device(y, x + 2, c), device(y + 2, x, c))
    other = device(y, x, 1 - c)
    barrier = pltpu.get_barrier_semaphore()
    for peer in up + down + opposite + (other,):
        pl.semaphore_signal(barrier, inc=1, device_id=peer, device_id_type=MESH)

    tokens, dim = h_ref.shape
    half = tokens // 2
    vocab = ea.shape[0] // (SIDE * CORES)
    wide = 512
    f32 = jnp.float32
    slots, span = ys.shape[0], CORES * vocab

    def remote(src, dst, send, recv, to):
        return pltpu.make_async_remote_copy(src_ref=src, dst_ref=dst, send_sem=send, recv_sem=recv, device_id=to, device_id_type=MESH)

    def xat(block, part=None):
        return xa.at[pl.ds(block * tokens, tokens)] if part is None else xa.at[pl.ds(block * tokens + part * half, half)]

    def eat(block, part=None):
        return ea.at[pl.ds(block * vocab, vocab)] if part is None else ea.at[pl.ds(block * vocab + part * (vocab // 2), vocab // 2)]

    def e_own(part):
        return e_any.at[pl.ds(part * (vocab // 2), vocab // 2)]

    tags = iter(range(gsend.shape[0]))

    def moving(src, dst, to):
        tag = next(tags)
        return remote(src, dst, gsend.at[tag], grecv.at[tag], to)

    def ring(own, at, unit, to_up, to_down):
        return [
            moving(own(0), at(unit, 0), to_up),
            moving(own(1), at(2 * unit, 1), to_down),
            moving(own(1), at(unit, 1), to_up),
            moving(own(0), at(2 * unit, 0), to_down),
            moving(at(unit, 0), at(3 * unit, 0), to_up),
            moving(at(2 * unit, 1), at(3 * unit, 1), to_down),
        ]

    gx = ring(lambda part: xat(0, part), xat, 1, up[0], down[0])
    ge = ring(e_own, eat, 2, up[1], down[1])
    swap = [
        moving(e_any, eat(1), other),
        moving(eat(2), eat(3), other),
        moving(eat(4), eat(5), other),
        moving(eat(6, 0), eat(7, 0), other),
        moving(eat(6, 1), eat(7, 1), other),
    ]
    codes = [
        moving(code_any, c_all.at[0, 0, 1], up[0]),
        moving(code_any, c_all.at[0, 0, 2], down[0]),
        moving(code_any, c_all.at[0, 0, 3], opposite[0]),
        moving(c_all.at[0, 0], c_all.at[0, 1], up[1]),
        moving(c_all.at[0, 0], c_all.at[0, 2], down[1]),
        moving(c_all.at[0, 0], c_all.at[0, 3], opposite[1]),
        moving(c_all.at[0], c_all.at[1], other),
    ]
    keep_e = pltpu.make_async_copy(e_any, eat(0), load.at[0])
    keep_c = pltpu.make_async_copy(code_any, c_all.at[0, 0, 0], load.at[1])
    keep_e.start()
    keep_c.start()
    pl.semaphore_wait(barrier, 7)
    for copy in ge[:4] + swap[:1] + codes[:3]:
        copy.start()
    step = half // 4

    def norm(i, carry):
        at = pl.ds(pl.multiple_of(i * step, step), step)
        x_hat, _ = normalize(h_ref[at, :])
        xa[at, :] = (x_hat * affine_ref[0:1, :] + affine_ref[1:2, :]).astype(xa.dtype)
        return carry

    lax.fori_loop(0, 8, norm, 0)

    halves = 2 * SIDE
    for slot in range(2):
        for hb in range(halves // 2):
            for kind, value in enumerate((-jnp.inf, 0.0, 0.0)):
                lane = (3 * hb + kind) * LANES
                ss[slot, :, lane:lane + LANES] = jnp.full((half, LANES), value, f32)
    for copy in gx[:4]:
        copy.start()
    keep_c.wait()
    for copy in codes[:3]:
        copy.wait_recv()
    for copy in codes[3:6]:
        copy.start()

    for block in range(SIDE):
        for r in range(tokens // LANES):
            hb, at = (block * tokens + r * LANES) // half, (r * LANES) % half
            more[0, at:at + LANES, hb * LANES:(hb + 1) * LANES] = jnp.broadcast_to(c_all[0, 0, block, r:r + 1, :].astype(f32), (LANES, LANES)).T

    def z_out(u, b, k, j):
        rows = pl.ds(pl.multiple_of(b * tokens + j * half, half), half)
        cols = pl.ds(pl.multiple_of(k * span, span), span)
        s = (2 * u) % slots + j
        return pltpu.make_async_copy(ys.at[s, :, pl.ds(0, span)], z_any.at[rows, cols], zsem.at[s])

    def logits(u, b, k):
        @pl.when(u >= 2)
        def _():
            for j in BOTH:
                z_out(u, b, k, j).wait()

        at = pl.ds(pl.multiple_of(b * tokens, tokens), tokens)
        s = (2 * u) % slots
        for n in range(span // span):
            ids_at = pl.ds(pl.multiple_of(k * span + n * span, span), span)
            e_at = pl.ds(pl.multiple_of(k * span + n * span, span), span)
            z = dot(xa[at, :], ea[e_at, :], 1, 1)
            ids = ids_ref[:, ids_at]
            for j in BOTH:
                zj = z[j * half:(j + 1) * half]
                ys[s + j, :, n * span:(n + 1) * span] = zj
                hb = 2 * b + j
                slot, lane = hb // SIDE, (hb % SIDE) * 3 * LANES
                lanes = [pl.ds(pl.multiple_of(lane + kind * LANES, LANES), LANES) for kind in range(3)]
                code = more[0, :, pl.ds(pl.multiple_of(hb * LANES, LANES), LANES)]
                old_max = ss[slot, :, lanes[0]]
                parts = [zj[:, g:g + LANES] for g in range(0, span, LANES)]
                new_max = functools.reduce(jnp.maximum, parts + [old_max])
                new_sum = ss[slot, :, lanes[1]] * jnp.exp(old_max - new_max)
                ss[slot, :, lanes[1]] = functools.reduce(jnp.add, [new_sum] + [jnp.exp(part - new_max) for part in parts])
                hits = [jnp.where(ids[:, g:g + LANES] == code, part, 0.0) for g, part in zip(range(0, span, LANES), parts)]
                ss[slot, :, lanes[2]] = functools.reduce(jnp.add, [ss[slot, :, lanes[2]]] + hits)
                ss[slot, :, lanes[0]] = new_max
        for j in BOTH:
            z_out(u, b, k, j).start()

    keep_e.wait()
    swap[0].wait_recv()
    logits(0, 0, 0)
    ge[0].wait_recv()
    ge[4].start()
    ge[1].wait_recv()
    ge[5].start()
    gx[0].wait_recv()
    gx[4].start()
    gx[1].wait_recv()
    gx[5].start()
    ge[2].wait_recv()
    swap[1].start()
    ge[3].wait_recv()
    swap[2].start()
    for copy in codes[3:6]:
        copy.wait_recv()
    codes[6].start()
    for copy in gx[2:4] + swap[1:3]:
        copy.wait_recv()

    def near(u, carry):
        logits(u, u // 3, u % 3)
        return carry

    lax.fori_loop(1, 8, near, 0)
    ge[4].wait_recv()
    swap[3].start()
    ge[5].wait_recv()
    swap[4].start()
    lax.fori_loop(8, 9, near, 0)
    gx[4].wait_recv()
    gx[5].wait_recv()

    def far_tokens(u, carry):
        logits(u, SIDE - 1, u - 9)
        return carry

    lax.fori_loop(9, 12, far_tokens, 0)
    swap[3].wait_recv()
    swap[4].wait_recv()

    def far_vocab(u, carry):
        logits(u, u - 12, SIDE - 1)
        return carry

    lax.fori_loop(12, 16, far_vocab, 0)
    codes[6].wait_recv()

    n_span = z_any.shape[1] // span
    per_block = 2 * n_span
    n_z = SIDE * per_block

    def spot(q):
        block, part = SIDE - 1 - q // per_block, (q // n_span) % 2
        return pl.multiple_of(block * tokens + part * half, half), pl.multiple_of((q % n_span) * span, span)

    def fetch(q):
        row, col = spot(q)
        return pltpu.make_async_copy(z_any.at[pl.ds(row, half), pl.ds(col, span)], ys.at[q % slots, :, pl.ds(0, span)], zsem.at[q % slots])

    for hb in range(halves):
        lanes = [slice((3 * (hb % SIDE) + kind) * LANES, (3 * (hb % SIDE) + kind + 1) * LANES) for kind in range(3)]
        run_max, run_sum, run_tgt = (ss[hb // SIDE, :, lane] for lane in lanes)
        peak = jnp.max(run_max, axis=1, keepdims=True)
        norm_sum = row_sum(run_sum * jnp.exp(run_max - peak))
        tgt = row_sum(run_tgt)
        lane = lax.broadcasted_iota(jnp.int32, (half, LANES), 1)
        stat_ref[:, hb * half:(hb + 1) * half] = jnp.where(lane == 0, peak, jnp.where(lane == 1, norm_sum, tgt)).T[:8, :]
    shifts = (1, -1, 2)
    stats = [remote(stat_ref, got.at[i], lsend.at[i], lrecv.at[i], peer) for i, peer in enumerate((up[0], down[0], opposite[0]))]
    for copy in stats:
        copy.start()
    count = row_sum(col_sum((c_all[...].reshape(-1, LANES) >= 0).astype(f32)))
    for j in BOTH:
        z_out(14, 0, 0, j).wait()
        z_out(15, 0, 0, j).wait()
    for q in range(slots - 1):
        fetch(q).start()
    for copy in gx + ge + swap + codes:
        copy.wait_send()
    for copy in stats:
        copy.wait_recv()
    line = lax.broadcasted_iota(jnp.int32, (LANES, half), 0)
    where_of = {o % SIDE: k for k, o in enumerate(OFFSETS)}
    for hb in range(halves):
        block, part = hb // 2, hb % 2
        views = [stat_ref[:, hb * half:(hb + 1) * half]]
        for i, shift in enumerate(shifts):
            at = (2 * where_of[(OFFSETS[block] + shift) % SIDE] + part) * half
            views.append(got[i, :, at:at + half])
        peak = functools.reduce(jnp.maximum, [v[0:1] for v in views])
        norm_sum = functools.reduce(jnp.add, [v[1:2] * jnp.exp(v[0:1] - peak) for v in views])
        tgt = functools.reduce(jnp.add, [v[2:3] for v in views])
        lse = peak + jnp.log(norm_sum)
        cols_ref[hb * half:(hb + 1) * half, :] = jnp.where(line == 0, lse, 0.0).T
        code = more[0, :, hb * LANES:(hb + 1) * LANES]
        lane = lax.broadcasted_iota(jnp.int32, (half, LANES), 1)
        weight = jnp.where(code >= 0, 1.0, 0.0)
        rest = jnp.where(lane == 1, weight / count, jnp.where(lane == 2, code, 0.0))
        cols_ref[hb * half:(hb + 1) * half, :] += rest
        if block == 0:
            weight_row = jnp.where(lane == 0, weight, 0.0).T[0:1, :]
            line8 = line[:8]
            rows_ref[:, part * half:(part + 1) * half] = jnp.where(line8 == 0, (lse - tgt) * weight_row, jnp.where(line8 == 1, count, 0.0))
    for copy in stats:
        copy.wait_send()

    def d_logits(q, carry):
        @pl.when(q + slots - 1 < n_z)
        def _():
            fetch(q + slots - 1).start()

        fetch(q).wait()
        row, col = spot(q)
        at = pl.ds(row, half)
        stat = cols_ref[at, :]
        lse, scale, code = (stat[:, k:k + 1] for k in range(3))
        for v in range(0, span, wide):
            here = pl.ds(pl.multiple_of(col + v, wide), wide)
            hot = jnp.where(ids_ref[:, here] == code, 1.0, 0.0)
            dz[at, here] = ((jnp.exp(ys[q % slots, :, v:v + wide] - lse) - hot) * scale).astype(dz.dtype)
        return carry

    lax.fori_loop(0, per_block, d_logits, 0)
    chunks = dim // wide

    def part_of(n):
        return pl.ds(pl.multiple_of(n * wide, wide), wide)

    def opening(kind, j, n):
        src, dst, to = ((xs, xr, (up, down)[j][0]), (ys, yr, (up, down)[j][1]), (ss, dr, other))[kind]
        tag = (kind * len(BOTH) + j) * chunks + n
        return remote(src.at[j, :, part_of(n)], dst.at[j, :, part_of(n)], osend.at[tag], orecv.at[tag], to)

    xc, yc, sc = ([[opening(kind, j, n) for n in range(chunks) for j in BOTH]] for kind in range(3))
    for p in range(1, SIDE):
        s = 2 * (p % 2)
        if p < SIDE - 1:
            xc.append([remote(xs.at[s + j], xr.at[2 * p + j], xsend.at[2 * p + j], xrecv.at[2 * p + j], (up, down)[j][0]) for j in BOTH])
            yc.append([remote(ys.at[s + j], yr.at[2 * p + j], ysend.at[2 * p + j], yrecv.at[2 * p + j], (up, down)[j][1]) for j in BOTH])
        sc.append([remote(ss.at[j], dr.at[2 * p + j], ssend.at[2 * p + j], srecv.at[2 * p + j], other) for j in BOTH])

    def two(ref, first):
        return [ref.at[first], ref.at[first + 1]]

    def add(dst, terms):
        copies = [pltpu.make_async_copy(ref, more.at[j], load.at[j]) for j, ref in enumerate(terms)]
        for copy in copies:
            copy.start()
        for copy in copies:
            copy.wait()
        for j in BOTH:
            dst[j][...] = dst[j][...] + more[j]

    def pick(j, pair):
        return jnp.where(j == 0, pair[0], pair[1])

    def x_tiles(p, s, first, last):
        at = [block * tokens + part * half for block, part in PHASES[p]]

        def tile(i, carry):
            j, n = i % 2, i // 2
            r = pl.ds(pl.multiple_of(pick(j, at), half), half)
            xs[s + j, :, part_of(n)] = dot(dz[r, :], ea[:, part_of(n)], 1, 0)
            return carry

        lax.fori_loop(2 * first, 2 * last, tile, 0)

    def y_tiles(p, core, out, s, first, last):
        part = vocab // 2
        at = [(block * CORES + core) * vocab + h * part for block, h in PHASES[p]]

        def tile(i, carry):
            j, n = i % 2, i // 2
            r = pl.ds(pl.multiple_of(pick(j, at), part), part)
            out[s + j, :, part_of(n)] = dot(dz[:, r], xa[:, part_of(n)], 0, 0)
            return carry

        lax.fori_loop(2 * first, 2 * last, tile, 0)

    def open_links(n, carry):
        x_tiles(0, 0, n, n + 1)
        for j in BOTH:
            opening(0, j, n).start()

        @pl.when(n == 0)
        def _():
            lax.fori_loop(per_block, n_z, d_logits, 0)

        y_tiles(0, 1, ss, 0, n, n + 1)
        for j in BOTH:
            opening(2, j, n).start()
        y_tiles(0, 0, ys, 0, n, n + 1)
        for j in BOTH:
            opening(2, j, n).wait_recv()
        copies = [pltpu.make_async_copy(dr.at[j, :, part_of(n)], more.at[j, :, part_of(n)], load.at[j]) for j in BOTH]
        for copy in copies:
            copy.start()
        for copy in copies:
            copy.wait()
        for j in BOTH:
            ys[j, :, part_of(n)] = ys[j, :, part_of(n)] + more[j, :, part_of(n)]
            opening(1, j, n).start()
        return carry

    lax.fori_loop(0, chunks, open_links, 0)
    for p in range(1, SIDE):
        s = 2 * (p % 2)
        if p >= 2:
            for copy in xc[p - 2]:
                copy.wait_send()
        x_tiles(p, s, 0, chunks)
        if p == 2:
            for copy in xc[0]:
                copy.wait_recv()
            add(two(xs, s), two(xr, 0))
        if p < 3:
            for copy in xc[p]:
                copy.start()
        for copy in sc[p - 1]:
            copy.wait_send()
        y_tiles(p, 1, ss, 0, 0, chunks)
        for copy in sc[p]:
            copy.start()
        if p >= 2:
            for copy in yc[p - 2]:
                copy.wait_send()
        y_tiles(p, 0, ys, s, 0, chunks)
        for copy in sc[p]:
            copy.wait_recv()
        add(two(ys, s), two(dr, 2 * p))
        if p == 2:
            for copy in yc[0]:
                copy.wait_recv()
            add(two(ys, s), two(yr, 0))
        if p < 3:
            for copy in yc[p]:
                copy.start()

    own_x, own_y = two(xs, 2), two(ys, 2)
    for own, landed, copies in ((own_x, xr, xc[1]), (own_y, yr, yc[1])):
        for copy in copies:
            copy.wait_recv()
        add(own, [landed.at[3], landed.at[2]])
    for copy in xc[2]:
        copy.wait_recv()
    add(own_x, two(xr, 4))
    step = half // 4
    sums_ref[...] = jnp.zeros(sums_ref.shape, jnp.float32)

    def norm_back(i, carry):
        j, r = i // 4, i % 4
        at = pl.ds(pl.multiple_of(i * step, step), step)
        d_normed = xs[2 + j, pl.ds(pl.multiple_of(r * step, step), step), :]
        x_hat, inv_std = normalize(h_ref[at, :])
        g = d_normed * affine_ref[0:1, :]
        centre, proj = row_mean(g), row_mean(g * x_hat)
        dh_ref[at, :] = (inv_std * (g - centre - x_hat * proj)).astype(dh_ref.dtype)
        sums_ref[0:1, :] += col_sum(d_normed * x_hat)
        sums_ref[1:2, :] += col_sum(d_normed)
        return carry

    lax.fori_loop(0, 8, norm_back, 0)
    sums_ref[2:3, 0:LANES] = functools.reduce(jnp.add, [rows_ref[0:1, g:g + LANES] for g in range(0, tokens, LANES)])

    stages = ((x, [device(y, x + d, c) for d in (1, -1, 2)]), (y, [device(y + d, x, c) for d in (1, -1, 2)]), (c, [other]))
    k = 0
    for stage, (pos, peers) in enumerate(stages):
        red[stage, pos] = sums_ref[...]
        copies = []
        for peer in peers:
            copies.append(remote(red.at[stage, pos], red.at[stage, pos], rsend.at[k], rrecv.at[k], peer))
            k += 1
        for copy in copies:
            copy.start()
        for copy in copies:
            copy.wait_recv()
        sums_ref[...] = functools.reduce(jnp.add, [red[stage, i] for i in range(len(peers) + 1)])
        for copy in copies:
            copy.wait_send()

    sums_ref[3:4, :] = jnp.broadcast_to(row_sum(sums_ref[2:3, 0:LANES]) / rows_ref[1:2, 0:1], (1, dim))

    for copy in yc[2]:
        copy.wait_recv()
    add(own_y, two(yr, 4))
    outs = [pltpu.make_async_copy(ys.at[2 + j], de_any.at[pl.ds(j * (vocab // 2), vocab // 2)], keep.at[j]) for j in BOTH]
    for copy in outs:
        copy.start()
    for copy in outs:
        copy.wait()
    for copy in xc[2] + yc[2] + sc[3]:
        copy.wait_send()


def step_call(hidden, embed, affine, code, ids):
    tokens, dim = hidden.shape
    vocab = embed.shape[0]
    n_tok, n_voc = SIDE * tokens, SIDE * CORES * vocab
    vmem, anywhere = pl.BlockSpec(memory_space=pltpu.VMEM), pl.BlockSpec(memory_space=pl.ANY)
    f32, bf16, tile = jnp.float32, jnp.bfloat16, (tokens // 2, dim)
    out = pl.pallas_call(
        step_kernel,
        out_shape=(
            jax.ShapeDtypeStruct(hidden.shape, bf16),
            jax.ShapeDtypeStruct((8, dim), f32),
            jax.ShapeDtypeStruct((8, tokens), f32),
            jax.ShapeDtypeStruct((vocab, dim), f32),
            jax.ShapeDtypeStruct((n_tok, n_voc), f32),
            jax.ShapeDtypeStruct((6,) + tile, f32),
            jax.ShapeDtypeStruct((6,) + tile, f32),
            jax.ShapeDtypeStruct((8,) + tile, f32),
        ),
        in_specs=[vmem, anywhere, vmem, anywhere, vmem],
        out_specs=(vmem, vmem, vmem) + (anywhere,) * 5,
        scratch_shapes=[
            pltpu.VMEM((n_tok, n_voc), bf16),
            pltpu.VMEM((n_tok, dim), bf16),
            pltpu.VMEM((n_voc, dim), bf16),
            pltpu.VMEM((4,) + tile, f32),
            pltpu.VMEM((4,) + tile, f32),
            pltpu.VMEM((2,) + tile, f32),
            pltpu.VMEM((2,) + tile, f32),
            pltpu.VMEM((3, SIDE, 8, dim), f32),
            pltpu.VMEM((n_tok, LANES), f32),
            pltpu.VMEM((CORES, SIDE, SIDE) + code.shape, jnp.int32),
            pltpu.VMEM((3, 8, n_tok), f32),
            pltpu.VMEM((8, n_tok), f32),
        ] + [pltpu.SemaphoreType.DMA((n,)) for n in (SIDE, SIDE, 24, 24, SIDE, SIDE) + (6,) * SIDE + (8,) * 5 + (18, 18)],
        compiler_params=pltpu.CompilerParams(collective_id=0, has_side_effects=True, vmem_limit_bytes=VMEM_LIMIT),
        cost_estimate=pl.CostEstimate(flops=6 * n_tok * n_voc * dim, bytes_accessed=10**8, transcendentals=2 * n_tok * n_voc),
    )(hidden, embed, affine, code, ids)
    return out[:4]


def solution(mesh):
    group = mesh.shape['tp']
    assert group == SIDE * SIDE * CORES

    def body(hidden, ln_gain, ln_bias, embed, targets, loss_mask):
        tokens, dim = hidden.shape
        vocab = embed.shape[0]
        rank = lax.axis_index('tp')
        y, x, c = rank // (SIDE * CORES), (rank // CORES) % SIDE, rank % CORES
        f32 = jnp.float32

        code = jnp.where(loss_mask > 0, targets, -1)
        code = jnp.pad(code.reshape(-1, LANES), ((0, 8 - tokens // LANES), (0, 0)), constant_values=-1)
        ids = column_ids(lax.broadcasted_iota(jnp.int32, (1, SIDE * CORES * vocab), 1), vocab, y, x, c).astype(f32)
        d_hidden, sums, rows, d_embed = step_call(hidden, embed, jnp.stack([ln_gain, ln_bias]), code, ids)
        own_loss = rows[0]
        return own_loss, sums[3, :1], d_hidden, d_embed, sums[0], sums[1]

    token_rows = P(('dp', 'tp'))
    token_mat = P(('dp', 'tp'), None)
    return jax.shard_map(body, mesh=mesh, in_specs=(token_mat, P(), P(), P('tp', None), token_rows, token_rows), out_specs=(token_rows, P('dp'), token_mat, token_mat, P('dp'), P('dp')), check_vma=False)
```
